32 devices in a mesh: col: 4 (over y, core), row: 8 (over z, x).
Axes of the slice: x: 2, y: 2, z: 4, core: 2. Of those that a mesh axis runs over, the one named last changes fastest.
Arguments:
- column_table: float32 [32768, 512], P('row', 'col'), may hold values from -3 to 3
- bag_rows: int32 [256, 32], P('row'), may hold values from 0 to 32767
Outputs:
- row_table: float32 [8, 4096, 512], P(None, ('col', 'row'))
- pooled: float32 [256, 512], P('row', 'col')
The draws below stay inside these ranges and needn't reach their ends.
Inputs may be any that keep to these rules, and one draw needn't show every extreme that they name: `bag_rows`: row indices of the table; a few rows are named far more often than the rest.
All inputs are finite; a program needn't handle non-finite values.
Results may differ from the reference program's by a relative error of at most 0.000078.
Values sent between devices are 32-bit elements; how exact they have to be, the bound alone decides.
No kernel may reach another device: no remote copies, remote signals or barrier semaphores. Data moves between devices by JAX's collectives and lax.ppermute only.
A program may use at most 64 MiB of HBM per device.

```python
import math
import jax
import jax.numpy as jnp
import numpy as np

E = 512
BAG_LEN = 32
ROWS = 32768
GROUPS = 8
BLOCK = 4096
BAGS = 256


def plant(drawn, own_key, low, top_value):
    place = [jax.random.randint(jax.random.fold_in(own_key, axis), (), 0, length) for axis, length in enumerate(drawn.shape)]
    longest = drawn.shape.index(max(drawn.shape))
    next_to = place[:longest] + [(place[longest] + 1) % drawn.shape[longest]] + place[longest + 1:]
    return drawn.at[tuple(place)].set(low).at[tuple(next_to)].set(top_value)


def steps_of(rng, shape, pieces, low, largest):
    gain = 1.0
    for position, shards_of in pieces:
        draws = jax.random.uniform(jax.random.fold_in(jax.random.fold_in(rng, 6), position), (shards_of,), jnp.float32, low / len(pieces), largest / len(pieces))
        gain = gain * jnp.repeat(jnp.exp(draws), shape[position] // shards_of).reshape((-1,) + (1,) * (len(shape) - 1 - position))
    return gain


def cumulative_ranks(count, lean):
    weights = [(1 << 20) // math.isqrt(grade ** lean) + 1 for grade in range(1, count + 1)]
    spread = 1 + sum(weights) // (1 << 30)
    return np.cumsum(np.array([max(1, weight // spread) for weight in weights]))


def ranked(own_key, dims, count, skew):
    table = cumulative_ranks(count, skew)
    lot = jax.random.randint(jax.random.fold_in(own_key, 1), dims, 0, int(table[count - 1]))
    standing = jnp.searchsorted(jnp.asarray(table, jnp.int32), lot, side="right")
    return jax.random.permutation(jax.random.fold_in(own_key, 2), count)[standing].astype(jnp.int32)


def bell_draw(rng, dims, scale, most, cuts=(), held_as=jnp.bfloat16):
    factor_of = steps_of(rng, dims, cuts, -0.22, 0.18) if cuts else 1.0
    values = jax.random.normal(rng, dims, jnp.float32) * scale * factor_of
    return jnp.minimum(jnp.maximum(values, -most), most).astype(held_as)


def setup_inputs(seed: int = 0) -> dict:
    key_list = jax.random.split(jax.random.key(seed), 3)
    column_table = bell_draw(key_list[0], (ROWS, E), 0.2, 3.0, ((0, 8), (1, 4)), jnp.float32)
    bag_rows = plant(ranked(key_list[1], (BAGS, BAG_LEN), ROWS, 2), jax.random.fold_in(key_list[1], 3), 0, ROWS - 1).astype(jnp.int32)
    return {"column_table": column_table, "bag_rows": bag_rows}


def reference(column_table, bag_rows):
    row_table = column_table.reshape(GROUPS, BLOCK, E)
    picked = jnp.take(column_table, bag_rows.reshape(-1), axis=0).reshape(BAGS, BAG_LEN, E)
    pooled = jnp.sum(picked.astype(jnp.float32), axis=1)
    return row_table, pooled
```

```python
import functools

import jax
import jax.numpy as jnp
from jax import lax
from jax.experimental import pallas as pl
from jax.experimental.pallas import tpu as pltpu
from jax.sharding import PartitionSpec as P

LANES = 128
SUB = 8
PACK = 2


def pool_kernel(first_ref, bags_ref, table_ref, out_ref, counts_ref):
    group_count, span = bags_ref.shape
    row_count, _ = table_ref.shape
    bag_len = span // SUB
    blocks = row_count // LANES
    first = first_ref[0]
    which = lax.broadcasted_iota(jnp.int32, (1, span), 1) // bag_len
    key_ids = lax.broadcasted_iota(jnp.int32, (blocks * SUB, span), 0)
    low_ids = lax.broadcasted_iota(jnp.int32, (LANES, span), 0)

    def count(index):
        within = bags_ref[pl.ds(index, 1), :] - first
        inside = (within >= 0) & (within < row_count)
        key = jnp.where(inside, (within >> 7) * SUB + which, -1)
        low = within & (LANES - 1)
        left = (key_ids == key).astype(jnp.float32).astype(jnp.bfloat16)
        right = (low_ids == low).astype(jnp.float32).astype(jnp.bfloat16)
        return lax.dot_general(
            left, right, (((1,), (1,)), ((), ())), preferred_element_type=jnp.float32
        )

    def fill(turn, _):
        parts = [count(turn * PACK + p) for p in range(PACK)]
        rows = pl.ds(pl.multiple_of(turn * PACK * SUB, PACK * SUB), PACK * SUB)
        for block in range(blocks):
            tile = jnp.concatenate(
                [part[block * SUB : (block + 1) * SUB, :] for part in parts], axis=0
            )
            counts_ref[rows, block * LANES : (block + 1) * LANES] = tile.astype(jnp.bfloat16)
        return 0

    lax.fori_loop(0, group_count // PACK, fill, 0)

    chunk = min(512, row_count)
    out_ref[...] = jnp.zeros_like(out_ref)

    def multiply(turn, _):
        place = pl.ds(pl.multiple_of(turn * chunk, chunk), chunk)
        rest = table_ref[place, :]
        left = counts_ref[:, place]
        total = out_ref[...]
        for _ in range(3):
            part = rest.astype(jnp.bfloat16)
            rest = rest - part.astype(jnp.float32)
            total += jnp.dot(left, part, preferred_element_type=jnp.float32)
        out_ref[...] = total
        return 0

    lax.fori_loop(0, row_count // chunk, multiply, 0)


def pool(first, bags, table):
    group_count, _ = bags.shape
    row_count, width = table.shape
    bag_count = group_count * SUB
    return pl.pallas_call(
        pool_kernel,
        out_shape=jax.ShapeDtypeStruct((bag_count, width), jnp.float32),
        in_specs=[
            pl.BlockSpec(memory_space=pltpu.SMEM),
            pl.BlockSpec(memory_space=pltpu.VMEM),
            pl.BlockSpec(memory_space=pltpu.VMEM),
        ],
        out_specs=pl.BlockSpec(memory_space=pltpu.VMEM),
        scratch_shapes=[pltpu.VMEM((bag_count, row_count), jnp.bfloat16)],
        cost_estimate=pl.CostEstimate(
            flops=20_000_000_000, bytes_accessed=4 * row_count * width, transcendentals=0
        ),
        name="pool",
    )(first, bags, table)


def place_kernel(cols, moved_ref, out_ref, sems):
    width = moved_ref.shape[-1]
    copies = []
    for c in range(cols):
        copies.append(
            pltpu.make_async_copy(
                moved_ref.at[c], out_ref.at[:, :, c * width : (c + 1) * width], sems.at[c]
            )
        )
    for copy in copies:
        copy.start()
    for copy in copies:
        copy.wait()


def place(moved):
    cols, rows, span, width = moved.shape
    if width % LANES:
        return moved.transpose(1, 2, 0, 3).reshape(rows, span, cols * width)
    return pl.pallas_call(
        functools.partial(place_kernel, cols),
        out_shape=jax.ShapeDtypeStruct((rows, span, cols * width), moved.dtype),
        in_specs=[pl.BlockSpec(memory_space=pl.ANY)],
        out_specs=pl.BlockSpec(memory_space=pl.ANY),
        scratch_shapes=[pltpu.SemaphoreType.DMA((cols,))],
        compiler_params=pltpu.CompilerParams(vmem_limit_bytes=1 << 20),
        name="place",
    )(moved)


def steps(column_table, bag_rows):
    rows = lax.axis_size("row")
    cols = lax.axis_size("col")
    block_len, width = column_table.shape
    own_bags, bag_len = bag_rows.shape
    span = block_len // (cols * rows)

    flat = bag_rows.reshape(1, own_bags // SUB, SUB * bag_len)
    every_bag = lax.all_to_all(
        jnp.broadcast_to(flat, (rows,) + flat.shape[1:]), "row", 0, 0, tiled=True
    ).reshape(rows * own_bags // SUB, SUB * bag_len)

    moved = lax.all_to_all(
        column_table.reshape(cols * rows, span, width), ("col", "row"), 0, 0, tiled=True
    )

    first = (lax.axis_index("row") * block_len).astype(jnp.int32).reshape(1)
    sums = pool(first, every_bag, column_table).reshape(rows, own_bags, width)
    pooled = jnp.sum(lax.all_to_all(sums, "row", 0, 0, tiled=True), axis=0)

    row_table = place(moved.reshape(cols, rows, span, width))
    return row_table, pooled


def solution(mesh):
    return jax.shard_map(
        steps,
        mesh=mesh,
        in_specs=(P("row", "col"), P("row", None)),
        out_specs=(P(None, ("col", "row"), None), P("row", "col")),
        check_vma=False,
    )
```
